32 devices in a mesh: dp: 8 (over y, x, core), mp: 4 (over z).
Axes of the slice: x: 2, y: 2, z: 4, core: 2. Of those that a mesh axis runs over, the one named last changes fastest.
Arguments:
- doc_ids: int32 [8, 512], P('dp'), may hold values from 0 to 128255
- doc_lengths: int32 [8], P('dp'), may hold values from 128 to 512
- activations: bfloat16 [4096, 4096], P('dp'), may hold values from -6 to 6
- out_grads: bfloat16 [4096, 14336], P('dp'), may hold values from -0.29882812 to 0.29882812
- input_basis: bfloat16 [4096, 2048], P(None, 'mp'), may hold values from -0.09375 to 0.09375
- output_basis: bfloat16 [14336, 7168], P('dp', 'mp'), may hold values from -0.046875 to 0.046875
- eigenvalues: bfloat16 [2048, 7168], P(None, 'mp'), may hold values from 0.5 to 50
- query_left: bfloat16 [32, 32, 2048], P('dp'), may hold values from -0.125 to 0.125
- query_right: bfloat16 [32, 32, 7168], P('dp', None, 'mp'), may hold values from -0.0625 to 0.0625
Outputs:
- scores: float32 [8, 32], P('dp')
The draws below stay inside these ranges and needn't reach their ends.
Inputs may be any that keep to these rules, and one draw needn't show every extreme that they name: `doc_lengths`: the live tokens are the first ones of each document.
All inputs are finite; a program needn't handle non-finite values.
Results may differ from the reference program's by a relative error of at most 0.023.
Values may be sent and summed in bfloat16 or wider, within the bound.
A program may use at most 192 MiB of HBM per device.

```python
import math
import jax
import jax.numpy as jnp
import numpy as np
from jax import lax

D = 4096
FF = 14336
VOCAB = 128256
KIN = 2048
KOUT = 7168
RANK = 32
DOC_LEN = 512
DOCS = 8
QUERIES = 32
TOKENS = 4096
N_DP = 8


def plant(drawn, stream_key, least, largest):
    dims = drawn.shape
    place = [jax.random.randint(jax.random.fold_in(stream_key, axis), (), 0, dims[axis]) for axis in range(len(dims))]
    drawn = drawn.at[tuple(place)].set(least)
    longest = dims.index(max(dims))
    place[longest] = (place[longest] + 1) % dims[longest]
    return drawn.at[tuple(place)].set(largest)


def levels(stream_key, dims, pieces, low, top_value):
    loudness = 1.0
    for axis_at, parts in pieces:
        draws = jax.random.uniform(jax.random.fold_in(jax.random.fold_in(stream_key, 6), axis_at), (parts,), jnp.float32, low / len(pieces), top_value / len(pieces))
        loudness = loudness * jnp.repeat(jnp.exp(draws), dims[axis_at] // parts).reshape((-1,) + (1,) * (len(dims) - 1 - axis_at))
    return loudness


def skewed_wide(stream_key, shape, number_of, skew):
    weights = [min(1 << octave, number_of + 1 - (1 << octave)) * (1 << 20) // math.isqrt((1 << octave) ** skew) + 1 for octave in range((number_of + 1).bit_length()) if 1 << octave <= number_of]
    scale = 1 + sum(weights) // (1 << 30)
    table = np.cumsum(np.array([max(1, weight // scale) for weight in weights]))
    pick = jax.random.randint(jax.random.fold_in(stream_key, 1), shape, 0, int(table[len(weights) - 1]))
    start = jnp.left_shift(1, jnp.searchsorted(jnp.asarray(table, jnp.int32), pick, side="right").astype(jnp.int32))
    grade = start - 1 + jax.random.randint(jax.random.fold_in(stream_key, 4), shape, 0, 1 << 30) % jnp.minimum(start, number_of + 1 - start)
    return jax.random.permutation(jax.random.fold_in(stream_key, 2), number_of)[grade].astype(jnp.int32)


def gaussian(own_key, extent, scale, reach, shards=(), held_as=jnp.bfloat16):
    result = jax.random.normal(own_key, extent, jnp.float32) * scale
    if len(shards) > 0:
        result = levels(own_key, extent, shards, -0.22, 0.18) * result
    return jnp.clip(result, min=-reach, max=reach).astype(held_as)


def setup_inputs(seed: int = 0) -> dict:
    key_of = jax.random.split(jax.random.key(seed), 10)
    doc_ids = plant(skewed_wide(key_of[0], (DOCS, DOC_LEN), VOCAB, 2), jax.random.fold_in(key_of[0], 3), 0, VOCAB - 1).astype(jnp.int32)
    doc_lengths = plant(jax.random.randint(key_of[1], (DOCS,), DOC_LEN // 4, DOC_LEN + 1), jax.random.fold_in(key_of[1], 1), DOC_LEN // 4, DOC_LEN).astype(jnp.int32)
    activations = gaussian(key_of[2], (TOKENS, D), 1.0, 6.0, ((0, 8),))
    out_grads = gaussian(key_of[3], (TOKENS, FF), 0.05, 0.29882812, ((0, 8),))
    input_basis = gaussian(key_of[4], (D, KIN), D ** -0.5, 0.09375, ((1, 4),))
    output_basis = gaussian(key_of[5], (FF, KOUT), FF ** -0.5, 0.046875, ((0, 8), (1, 4)))
    eigenvalues = jnp.clip(jnp.exp(math.log(50.0) - 4.6051702 * jax.random.uniform(key_of[6], (KIN, KOUT), jnp.float32) ** levels(key_of[6], (KIN, KOUT), ((1, 4),), -0.2, 0.2)), 0.5, 50.0).astype(jnp.bfloat16)
    query_left = gaussian(key_of[7], (QUERIES, RANK, KIN), KIN ** -0.5, 0.125, ((0, 8),))
    query_right = gaussian(key_of[8], (QUERIES, RANK, KOUT), KOUT ** -0.5, 0.0625, ((0, 8), (2, 4)))
    return {"doc_ids": doc_ids, "doc_lengths": doc_lengths, "activations": activations, "out_grads": out_grads, "input_basis": input_basis, "output_basis": output_basis, "eigenvalues": eigenvalues, "query_left": query_left, "query_right": query_right}


damping = 0.5


def token_weights(doc_ids, doc_lengths):
    positions = jnp.arange(doc_ids.shape[1], dtype=jnp.int32)
    active = positions[None, :] < doc_lengths[:, None]
    matches = (doc_ids[:, :, None] == doc_ids[:, None, :]) & active[:, None, :]
    repeats = jnp.sum(matches.astype(jnp.float32), axis=2)
    return jnp.where(active, 1.0 / jnp.maximum(repeats, 1.0), 0.0).astype(jnp.float32)


def reference(doc_ids, doc_lengths, activations, out_grads, input_basis, output_basis, eigenvalues, query_left, query_right):
    rotated_in = jnp.dot(activations, input_basis, preferred_element_type=jnp.float32).astype(jnp.bfloat16)
    width = FF // N_DP
    summed = jnp.zeros((TOKENS, KOUT), jnp.float32)
    for member in range(N_DP):
        partial_value = jnp.dot(out_grads[:, member * width:(member + 1) * width], output_basis[member * width:(member + 1) * width], preferred_element_type=jnp.float32)
        summed = summed + lax.optimization_barrier(partial_value.astype(jnp.bfloat16)).astype(jnp.float32)
    rotated_out = summed.astype(jnp.bfloat16)
    weights = token_weights(doc_ids, doc_lengths)
    left_rows = query_left.reshape(QUERIES * RANK, KIN)
    right_rows = query_right.reshape(QUERIES * RANK, KOUT).astype(jnp.float32)
    denominator = eigenvalues.astype(jnp.float32) + damping

    def per_document(doc_index):
        first = doc_index * DOC_LEN
        acts_doc = lax.dynamic_slice_in_dim(rotated_in, first, DOC_LEN, 0)
        grads_doc = lax.dynamic_slice_in_dim(rotated_out, first, DOC_LEN, 0)
        weight_doc = lax.dynamic_index_in_dim(weights, doc_index, 0, keepdims=False)
        scaled = (weight_doc[:, None] * grads_doc.astype(jnp.float32)).astype(jnp.bfloat16)
        gradient = jnp.dot(acts_doc.T, scaled, preferred_element_type=jnp.float32)
        conditioned = (gradient / denominator).astype(jnp.bfloat16)
        mixture = jnp.dot(left_rows, conditioned, preferred_element_type=jnp.float32)
        return jnp.sum((mixture * right_rows).reshape(QUERIES, RANK * KOUT), axis=1)

    return lax.map(per_document, jnp.arange(DOCS, dtype=jnp.int32))
```

```python
import functools

import jax
import jax.numpy as jnp
from jax import lax
from jax.sharding import PartitionSpec as P

damping = 0.5


def token_weights(doc_ids, doc_lengths):
    positions = jnp.arange(doc_ids.shape[1], dtype=jnp.int32)
    active = positions[None, :] < doc_lengths[:, None]
    matches = (doc_ids[:, :, None] == doc_ids[:, None, :]) & active[:, None, :]
    repeats = jnp.sum(matches.astype(jnp.float32), axis=2)
    return jnp.where(active, 1.0 / jnp.maximum(repeats, 1.0), 0.0)


def column_pieces(columns, unit=256, pieces=4):
    units = -(-columns // unit)
    pieces = min(pieces, units)
    bounds = [0]
    for k in range(pieces):
        bounds.append(bounds[-1] + units // pieces + (1 if k < units % pieces else 0))
    return [(a * unit, min(b * unit, columns)) for a, b in zip(bounds[:-1], bounds[1:])]


def per_device(
    n_dp,
    n_mp,
    doc_ids,
    doc_lengths,
    activations,
    out_grads,
    input_basis,
    output_basis,
    eigenvalues,
    query_left,
    query_right,
):
    groups = n_dp // 4
    index = lax.axis_index("dp")
    group, place = index // 4, index % 4

    def swap(value, bit):
        return lax.ppermute(value, "dp", [(j, j ^ bit) for j in range(n_dp)])

    def shift(value, steps):
        return lax.ppermute(value, "dp", [(j, (j + 4 * steps) % n_dp) for j in range(n_dp)])

    depth, out_cols = output_basis.shape
    tokens = out_grads.shape[0]
    pieces = column_pieces(out_cols)

    def over_groups(blocks):
        return jnp.concatenate([blocks] + [shift(blocks, s) for s in range(1, groups)], axis=1)

    def over_bit(blocks, bit):
        return jnp.concatenate([blocks, swap(blocks, bit)], axis=0)

    left = over_groups(over_bit(query_left[None, None], 2))
    right = over_bit(over_groups(query_right[None, None]), 2)

    pair_left, pair_right = left, right

    def following(value):
        return lax.optimization_barrier((value, pair_left, pair_right))[0]

    own_pieces = following([output_basis[:, low:high] for low, high in pieces])
    left, right = over_bit(left, 1), over_bit(right, 1)
    per_block, rank_rows = query_left.shape[0], query_left.shape[1]
    number = n_dp * per_block
    left_rows = left.reshape(number * rank_rows, query_left.shape[2])
    right_rows = right.reshape(number * rank_rows, out_cols)

    basis = []
    partner = swap(output_basis, 1)
    for (low, high), own in zip(pieces, own_pieces):
        basis.append([output_basis[:, low:high], partner[:, low:high], swap(own, 2)])

    shared = tokens // 2
    part = shared // n_mp
    direct = tokens - shared

    def columns_of(to_group, q, first, rows):
        start = (to_group * 4 + (place ^ q)) * depth
        return lax.dynamic_slice(out_grads, (first, start), (rows, depth))

    mine = [columns_of(group, q, 0, tokens) for q in range(4)]
    others = []
    first = direct + lax.axis_index("mp") * part
    for s in range(1, groups):
        to_group = (group + s) % groups
        got = [[None, None] for _ in range(4)]
        for q in range(4):
            piece = shift(columns_of(to_group, q, first, part), s)
            got[q][1] = piece
        both = lax.all_gather(jnp.stack([g[1] for g in got]), "mp", axis=1, tiled=True)
        for q in range(4):
            got[q][0] = shift(following(columns_of(to_group, q, 0, direct)), s)
            got[q][1] = both[q]
        others.append(got)

    rotated_share = jnp.dot(activations, input_basis, preferred_element_type=jnp.float32).astype(
        jnp.bfloat16
    )
    rotated_in = lax.all_gather(rotated_share, "mp", axis=1, tiled=True)

    weights = token_weights(doc_ids, doc_lengths)
    docs_here = doc_ids.shape[0]
    acts_doc = rotated_in.reshape(docs_here, -1, rotated_in.shape[1])

    def product(rows_of, blocks):
        total = jnp.dot(rows_of[0], blocks[0], preferred_element_type=jnp.float32)
        for q in range(1, 4):
            total = total + jnp.dot(rows_of[q], blocks[q], preferred_element_type=jnp.float32)
        return total

    values = jnp.zeros((docs_here, number), jnp.float32)
    sent, done = (), [values]
    for (low, high), blocks in zip(pieces, basis):
        across = lax.optimization_barrier((blocks[2], sent, tuple(done[:-1])))[0]
        blocks = [blocks[0], blocks[1], across, swap(across, 1)]
        came, sent = [], ()
        for s in range(1, groups):
            halves = [product([g[k] for g in others[s - 1]], blocks) for k in range(2)]
            part_sum = jnp.concatenate(halves, axis=0).astype(jnp.bfloat16)
            sent = sent + (part_sum,)
            came.append(shift(part_sum, groups - s))
        summed = product(mine, blocks).astype(jnp.bfloat16).astype(jnp.float32)
        for other in came:
            summed = summed + other.astype(jnp.float32)
        grads_doc = summed.astype(jnp.bfloat16).reshape(docs_here, -1, high - low)
        scaled = (weights[:, :, None] * grads_doc.astype(jnp.float32)).astype(jnp.bfloat16)
        gradient = jnp.einsum("dti,dtj->dij", acts_doc, scaled, preferred_element_type=jnp.float32)
        denominator = eigenvalues[:, low:high].astype(jnp.float32) + damping
        conditioned = (gradient / denominator).astype(jnp.bfloat16)
        mixture = jnp.einsum("ri,dij->drj", left_rows, conditioned, preferred_element_type=jnp.float32)
        weighted = mixture * right_rows[None, :, low:high].astype(jnp.float32)
        values = values + jnp.sum(weighted.reshape(docs_here, number, -1), axis=2)
        done.append(values)
    values = lax.psum(values, "mp")

    at = jnp.arange(n_dp, dtype=jnp.int32)
    slot, back = at // groups, at % groups
    q_of = (slot % 2) * 2 + slot // 2
    holder = ((group - back) % groups) * 4 + (place ^ q_of)
    same = holder[:, None] == at[None, :]
    spread = values.reshape(docs_here, n_dp, 1, per_block)
    placed = jnp.sum(jnp.where(same[None, :, :, None], spread, 0.0), axis=1)
    return placed.reshape(docs_here, number)


def solution(mesh):
    return jax.shard_map(
        functools.partial(per_device, mesh.shape["dp"], mesh.shape["mp"]),
        mesh=mesh,
        in_specs=(
            P("dp", None),
            P("dp"),
            P("dp", None),
            P("dp", None),
            P(None, "mp"),
            P("dp", "mp"),
            P(None, "mp"),
            P("dp", None, None),
            P("dp", None, "mp"),
        ),
        out_specs=P("dp", None),
        check_vma=False,
    )
```
